32 devices in a mesh: data: 8 (over z, y), width: 4 (over x, core).
Axes of the slice: x: 2, y: 2, z: 4, core: 2. Of those that a mesh axis runs over, the one named last changes fastest.
Arguments:
- grad_up: float32 [8, 768, 3072], P('data', None, 'width'), may hold values from -4 to 4
- grad_down: float32 [8, 3072, 768], P('data', 'width'), may hold values from -4 to 4
- grad_query: float32 [8, 768, 768], P('data', None, 'width'), may hold values from -4 to 4
- grad_key: float32 [8, 768, 768], P('data', None, 'width'), may hold values from -4 to 4
- grad_value: float32 [8, 768, 768], P('data', None, 'width'), may hold values from -4 to 4
- grad_mixed: float32 [8, 768, 768], P('data', 'width'), may hold values from -4 to 4
- grad_norm: float32 [8, 768], P('data'), may hold values from -8 to 8
- weight_up: float32 [768, 3072], P('data', 'width'), may hold values from -0.21875 to 0.21875
- weight_down: float32 [3072, 768], P('width', 'data'), may hold values from -0.109375 to 0.109375
- weight_query: float32 [768, 768], P('data', 'width'), may hold values from -0.21875 to 0.21875
- weight_key: float32 [768, 768], P('data', 'width'), may hold values from -0.21875 to 0.21875
- weight_value: float32 [768, 768], P('data', 'width'), may hold values from -0.21875 to 0.21875
- weight_mixed: float32 [768, 768], P('width', 'data'), may hold values from -0.21875 to 0.21875
- weight_norm: float32 [768], P('data'), may hold values from 0.25 to 1.75
- moment_up: float32 [768, 3072], P('data', 'width'), may hold values from 0.05 to 0.8
- moment_down: float32 [3072, 768], P('width', 'data'), may hold values from 0.05 to 0.8
- moment_query: float32 [768, 768], P('data', 'width'), may hold values from 0.05 to 0.8
- moment_key: float32 [768, 768], P('data', 'width'), may hold values from 0.05 to 0.8
- moment_value: float32 [768, 768], P('data', 'width'), may hold values from 0.05 to 0.8
- moment_mixed: float32 [768, 768], P('width', 'data'), may hold values from 0.05 to 0.8
- moment_norm: float32 [768], P('data'), may hold values from 0.05 to 0.8
Outputs:
- copy_up: bfloat16 [768, 3072], P(None, 'width')
- copy_down: bfloat16 [3072, 768], P('width')
- copy_query: bfloat16 [768, 768], P(None, 'width')
- copy_key: bfloat16 [768, 768], P(None, 'width')
- copy_value: bfloat16 [768, 768], P(None, 'width')
- copy_mixed: bfloat16 [768, 768], P('width')
- copy_norm: bfloat16 [768], replicated
- new_up: float32 [768, 3072], P('data', 'width')
- new_down: float32 [3072, 768], P('width', 'data')
- new_query: float32 [768, 768], P('data', 'width')
- new_key: float32 [768, 768], P('data', 'width')
- new_value: float32 [768, 768], P('data', 'width')
- new_mixed: float32 [768, 768], P('width', 'data')
- new_norm: float32 [768], P('data')
- state_new_up: float32 [768, 3072], P('data', 'width')
- state_new_down: float32 [3072, 768], P('width', 'data')
- state_new_query: float32 [768, 768], P('data', 'width')
- state_new_key: float32 [768, 768], P('data', 'width')
- state_new_value: float32 [768, 768], P('data', 'width')
- state_new_mixed: float32 [768, 768], P('width', 'data')
- state_new_norm: float32 [768], P('data')
The draws below stay inside these ranges and needn't reach their ends.
All inputs are finite; a program needn't handle non-finite values.
Results may differ from the reference program's by a relative error of at most 0.0004.
Values may be sent and summed in bfloat16 or wider, within the bound.
A program may use at most 128 MiB of HBM per device.

```python
import jax
import jax.numpy as jnp
from jax import lax

WIDTH = 768
INNER = 3072
ATTN = 768
REPLICAS = 8


def raised(entries, stream_key, source, target, parts, factor):
    owner, partner = [(jnp.arange(entries.shape[axis_at]) // (entries.shape[axis_at] // parts)).reshape([-1 if axis == axis_at else 1 for axis in range(entries.ndim)]) for axis_at in (source, target)]
    chosen = jax.random.permutation(stream_key, parts)[partner]
    strong = (owner == chosen) | (owner == (partner + parts // 2) % parts)
    return jnp.where(strong, factor * entries, entries)


def block_scale(key, dims, split, smallest, largest):
    def one(dim, shards_of):
        draws = jax.random.uniform(jax.random.fold_in(jax.random.fold_in(key, 6), dim), (shards_of,), jnp.float32, smallest / len(split), largest / len(split))
        return jnp.repeat(jnp.exp(draws), dims[dim] // shards_of).reshape((-1,) + (1,) * (len(dims) - dim - 1))

    loudness = one(*split[0])
    for cut in split[1:]:
        loudness = loudness * one(*cut)
    return loudness


def scatter_about(own_key, extent, deviation, reach, split=(), held_as=jnp.bfloat16):
    factor_of = block_scale(own_key, extent, split, -0.22, 0.18) if split else 1.0
    drawn = jax.random.normal(own_key, extent, jnp.float32) * deviation * factor_of
    return jnp.minimum(jnp.maximum(drawn, -reach), reach).astype(held_as)


def noise_with(rng, dims, width, reach, pieces, heavy, kind=jnp.bfloat16):
    drawn = width * jax.random.normal(rng, dims, jnp.float32)
    if pieces:
        drawn = drawn * block_scale(rng, dims, pieces, -0.22, 0.18)
    return jnp.clip(raised(drawn, jax.random.fold_in(rng, 3), *heavy), -reach, reach).astype(kind)


def setup_inputs(seed: int = 0) -> dict:
    keys = jax.random.split(jax.random.key(seed), 22)
    grad_up = noise_with(keys[0], (REPLICAS, WIDTH, INNER), 0.5, 4.0, ((0, 8), (2, 4)), (0, 1, 8, 2.0), jnp.float32)
    grad_down = noise_with(keys[1], (REPLICAS, INNER, WIDTH), 0.5, 4.0, ((0, 8), (1, 4)), (0, 2, 8, 2.0), jnp.float32)
    grad_query = noise_with(keys[2], (REPLICAS, WIDTH, ATTN), 0.5, 4.0, ((0, 8), (2, 4)), (0, 1, 8, 2.0), jnp.float32)
    grad_key = noise_with(keys[3], (REPLICAS, WIDTH, ATTN), 0.5, 4.0, ((0, 8), (2, 4)), (0, 1, 8, 2.0), jnp.float32)
    grad_value = noise_with(keys[4], (REPLICAS, WIDTH, ATTN), 0.5, 4.0, ((0, 8), (2, 4)), (0, 1, 8, 2.0), jnp.float32)
    grad_mixed = noise_with(keys[5], (REPLICAS, ATTN, WIDTH), 0.5, 4.0, ((0, 8), (1, 4)), (0, 2, 8, 2.0), jnp.float32)
    grad_norm = noise_with(keys[6], (REPLICAS, WIDTH), 1.0, 8.0, ((0, 8),), (0, 1, 8, 2.0), jnp.float32)
    weight_up = scatter_about(keys[7], (WIDTH, INNER), WIDTH ** -0.5, 0.21875, ((0, 8), (1, 4)), jnp.float32)
    weight_down = scatter_about(keys[8], (INNER, WIDTH), INNER ** -0.5, 0.109375, ((0, 4), (1, 8)), jnp.float32)
    weight_query = scatter_about(keys[9], (WIDTH, ATTN), WIDTH ** -0.5, 0.21875, ((0, 8), (1, 4)), jnp.float32)
    weight_key = scatter_about(keys[10], (WIDTH, ATTN), WIDTH ** -0.5, 0.21875, ((0, 8), (1, 4)), jnp.float32)
    weight_value = scatter_about(keys[11], (WIDTH, ATTN), WIDTH ** -0.5, 0.21875, ((0, 8), (1, 4)), jnp.float32)
    weight_mixed = scatter_about(keys[12], (ATTN, WIDTH), ATTN ** -0.5, 0.21875, ((0, 4), (1, 8)), jnp.float32)
    weight_norm = jnp.clip(1.0 + 0.15 * jax.random.normal(keys[13], (WIDTH,), jnp.float32), 0.25, 1.75)
    moment_up = jnp.clip(0.05 + 0.75 * jax.random.uniform(keys[14], (WIDTH, INNER), jnp.float32) ** block_scale(keys[14], (WIDTH, INNER), ((0, 8), (1, 4)), -0.2, 0.2), 0.05, 0.8)
    moment_down = jnp.clip(0.05 + 0.75 * jax.random.uniform(keys[15], (INNER, WIDTH), jnp.float32) ** block_scale(keys[15], (INNER, WIDTH), ((0, 4), (1, 8)), -0.2, 0.2), 0.05, 0.8)
    moment_query = jnp.clip(0.05 + 0.75 * jax.random.uniform(keys[16], (WIDTH, ATTN), jnp.float32) ** block_scale(keys[16], (WIDTH, ATTN), ((0, 8), (1, 4)), -0.2, 0.2), 0.05, 0.8)
    moment_key = jnp.clip(0.05 + 0.75 * jax.random.uniform(keys[17], (WIDTH, ATTN), jnp.float32) ** block_scale(keys[17], (WIDTH, ATTN), ((0, 8), (1, 4)), -0.2, 0.2), 0.05, 0.8)
    moment_value = jnp.clip(0.05 + 0.75 * jax.random.uniform(keys[18], (WIDTH, ATTN), jnp.float32) ** block_scale(keys[18], (WIDTH, ATTN), ((0, 8), (1, 4)), -0.2, 0.2), 0.05, 0.8)
    moment_mixed = jnp.clip(0.05 + 0.75 * jax.random.uniform(keys[19], (ATTN, WIDTH), jnp.float32) ** block_scale(keys[19], (ATTN, WIDTH), ((0, 4), (1, 8)), -0.2, 0.2), 0.05, 0.8)
    moment_norm = jnp.clip(0.05 + 0.75 * jax.random.uniform(keys[20], (WIDTH,), jnp.float32) ** block_scale(keys[20], (WIDTH,), ((0, 8),), -0.2, 0.2), 0.05, 0.8)
    return dict(grad_up=grad_up, grad_down=grad_down, grad_query=grad_query, grad_key=grad_key, grad_value=grad_value, grad_mixed=grad_mixed, grad_norm=grad_norm, weight_up=weight_up, weight_down=weight_down, weight_query=weight_query, weight_key=weight_key, weight_value=weight_value, weight_mixed=weight_mixed, weight_norm=weight_norm, moment_up=moment_up, moment_down=moment_down, moment_query=moment_query, moment_key=moment_key, moment_value=moment_value, moment_mixed=moment_mixed, moment_norm=moment_norm)


learn_rate = 0.05
hold_rate = 0.9

def reference(grad_up, grad_down, grad_query, grad_key, grad_value, grad_mixed, grad_norm, weight_up, weight_down, weight_query, weight_key, weight_value, weight_mixed, weight_norm, moment_up, moment_down, moment_query, moment_key, moment_value, moment_mixed, moment_norm):
    mean_up = lax.optimization_barrier(jnp.sum(grad_up.astype(jnp.float32), axis=0)) * REPLICAS ** (-0.5)
    mean_down = lax.optimization_barrier(jnp.sum(grad_down.astype(jnp.float32), axis=0)) * REPLICAS ** (-0.5)
    mean_query = lax.optimization_barrier(jnp.sum(grad_query.astype(jnp.float32), axis=0)) * REPLICAS ** (-0.5)
    mean_key = lax.optimization_barrier(jnp.sum(grad_key.astype(jnp.float32), axis=0)) * REPLICAS ** (-0.5)
    mean_value = lax.optimization_barrier(jnp.sum(grad_value.astype(jnp.float32), axis=0)) * REPLICAS ** (-0.5)
    mean_mixed = lax.optimization_barrier(jnp.sum(grad_mixed.astype(jnp.float32), axis=0)) * REPLICAS ** (-0.5)
    mean_norm = lax.optimization_barrier(jnp.sum(grad_norm.astype(jnp.float32), axis=0)) * REPLICAS ** (-0.5)
    state_new_up = hold_rate * moment_up + (1.0 - hold_rate) * mean_up * mean_up
    new_up = weight_up - learn_rate * mean_up * lax.rsqrt(state_new_up + 1e-06)
    state_new_down = hold_rate * moment_down + (1.0 - hold_rate) * mean_down * mean_down
    new_down = weight_down - learn_rate * mean_down * lax.rsqrt(state_new_down + 1e-06)
    state_new_query = hold_rate * moment_query + (1.0 - hold_rate) * mean_query * mean_query
    new_query = weight_query - learn_rate * mean_query * lax.rsqrt(state_new_query + 1e-06)
    state_new_key = hold_rate * moment_key + (1.0 - hold_rate) * mean_key * mean_key
    new_key = weight_key - learn_rate * mean_key * lax.rsqrt(state_new_key + 1e-06)
    state_new_value = hold_rate * moment_value + (1.0 - hold_rate) * mean_value * mean_value
    new_value = weight_value - learn_rate * mean_value * lax.rsqrt(state_new_value + 1e-06)
    state_new_mixed = hold_rate * moment_mixed + (1.0 - hold_rate) * mean_mixed * mean_mixed
    new_mixed = weight_mixed - learn_rate * mean_mixed * lax.rsqrt(state_new_mixed + 1e-06)
    state_new_norm = hold_rate * moment_norm + (1.0 - hold_rate) * mean_norm * mean_norm
    new_norm = weight_norm - learn_rate * mean_norm * lax.rsqrt(state_new_norm + 1e-06)
    copy_up = new_up.astype(jnp.bfloat16)
    copy_down = new_down.astype(jnp.bfloat16)
    copy_query = new_query.astype(jnp.bfloat16)
    copy_key = new_key.astype(jnp.bfloat16)
    copy_value = new_value.astype(jnp.bfloat16)
    copy_mixed = new_mixed.astype(jnp.bfloat16)
    copy_norm = new_norm.astype(jnp.bfloat16)
    return (copy_up, copy_down, copy_query, copy_key, copy_value, copy_mixed, copy_norm, new_up, new_down, new_query, new_key, new_value, new_mixed, new_norm, state_new_up, state_new_down, state_new_query, state_new_key, state_new_value, state_new_mixed, state_new_norm)
```

```python
import functools

import jax
import jax.numpy as jnp
from jax import lax
from jax.experimental import pallas as pl
from jax.experimental.pallas import tpu as pltpu
from jax.sharding import PartitionSpec as P

learn_rate = 0.05
hold_rate = 0.9
LANES = 128
SUB = 8


def round_up(value, unit):
    return -(-value // unit) * unit


def turn(block):
    rows, cols = block.shape
    tall, wide = round_up(rows, LANES), round_up(cols, LANES)
    if wide != cols:
        block = jnp.concatenate([block, jnp.zeros((rows, wide - cols), block.dtype)], axis=1)
    if tall != rows:
        block = jnp.concatenate([block, jnp.zeros((tall - rows, wide), block.dtype)], axis=0)
    return block.T[:cols, :rows]


def kernel(n, bits, rows, orders, *refs):
    refs = list(refs)
    take = lambda count: [refs.pop(0) for _ in range(count)]
    g_up, g_down, g_query, g_key, g_value, g_mixed, g_norm = take(7)
    w_up, w_down, w_query, w_key, w_value, w_mixed, w_norm = take(7)
    m_up, m_down, m_query, m_key, m_value, m_mixed, m_norm = take(7)
    c_up, c_down, c_query, c_key, c_value, c_mixed, c_norm = take(7)
    n_up, n_down, n_query, n_key, n_value, n_mixed, n_norm = take(7)
    s_up, s_down, s_query, s_key, s_value, s_mixed, s_norm = take(7)
    count = len(orders)
    part = take(count)
    held = [take(bits) for _ in range(count)]
    copies = take(count)
    send_sem, recv_sem = take(2)

    me = lax.axis_index("data")
    bit = [(me // 2**k) % 2 for k in range(bits)]
    partner = [me + 2**k * (1 - 2 * bit[k]) for k in range(bits)]

    barrier = pltpu.get_barrier_semaphore()
    for k in range(bits):
        pl.semaphore_signal(
            barrier, inc=1, device_id={"data": partner[k]}, device_id_type=pl.DeviceIdType.MESH
        )
    pl.semaphore_wait(barrier, bits)

    mean_rate = n ** (-0.5)
    half = g_up.shape[1] // 2
    heads = g_query.shape[1]
    mine = tuple(bit[k] for k in reversed(range(bits)))
    every = (slice(None),) * bits

    def index(chunk, step, own):
        fixed = {k: bit[k] for k in orders[chunk][:step]}
        if step < bits:
            k = orders[chunk][step]
            fixed[k] = bit[k] if own else 1 - bit[k]
        return tuple(fixed.get(k, slice(None)) for k in reversed(range(bits)))

    def copy(src, dst, chunk, slot, k):
        return pltpu.make_async_remote_copy(
            src_ref=src,
            dst_ref=dst,
            send_sem=send_sem.at[chunk, slot],
            recv_sem=recv_sem.at[chunk, slot],
            device_id={"data": partner[k]},
            device_id_type=pl.DeviceIdType.MESH,
        )

    def scatter(chunk, step):
        return copy(
            part[chunk].at[index(chunk, step, False)],
            held[chunk][step],
            chunk,
            step,
            orders[chunk][step],
        )

    def gather(chunk, step):
        there = copies[chunk].at[index(chunk, step, True)]
        return copy(there, there, chunk, bits + step, orders[chunk][step])

    def tile_loop(body):
        def step(i, carry):
            body(pl.multiple_of(i * SUB, SUB))
            return carry

        lax.fori_loop(0, rows // SUB, step, 0)

    def blocks(value):
        return value.reshape((2,) * bits + (rows, value.shape[-1]))

    def fill_up(h):
        def fill(chunk):
            for d in range(n):
                where = tuple((d >> k) & 1 for k in reversed(range(bits)))

                def body(r):
                    part[chunk][where + (pl.ds(r, SUB), slice(None))] = g_up[
                        pl.ds(pl.multiple_of(d * rows + r, SUB), SUB), h * half : (h + 1) * half
                    ]

                tile_loop(body)

        return fill

    def fill_down(h):
        def fill(chunk):
            for j in range(half // LANES):
                block = g_down[h * half + j * LANES : h * half + (j + 1) * LANES, :]
                part[chunk][every + (slice(None), slice(j * LANES, (j + 1) * LANES))] = blocks(turn(block))

        return fill

    def fill_pair(first, second, turned):
        def fill(chunk):
            for d in range(n):
                where = tuple((d >> k) & 1 for k in reversed(range(bits)))
                if turned is None:

                    def body(r):
                        at = pl.ds(pl.multiple_of(d * rows + r, SUB), SUB)
                        part[chunk][where + (pl.ds(r, SUB), slice(None))] = jnp.concatenate(
                            [first[at, :], second[at, :]], axis=1
                        )

                    tile_loop(body)
                else:
                    at = slice(d * rows, (d + 1) * rows)
                    part[chunk][where] = jnp.concatenate([first[at, :], turned[at, :]], axis=1)

        return fill

    def fill_norm(chunk):
        for d in range(n):
            where = tuple((d >> k) & 1 for k in reversed(range(bits)))
            part[chunk][where] = jnp.zeros_like(part[chunk][where])
            part[chunk][where + (slice(0, 1), slice(0, rows))] = g_norm[d : d + 1, :]

    def update(total, weight, moment):
        mean = total * mean_rate
        state = hold_rate * moment + (1.0 - hold_rate) * mean * mean
        return weight - learn_rate * mean * lax.rsqrt(state + 1e-06), state

    def own(chunk, lanes):
        return part[chunk][mine + (slice(None), lanes)]

    def step_up(h):
        def run(chunk):
            at = slice(h * half, (h + 1) * half)
            new, state = update(own(chunk, slice(None)), w_up[:, at], m_up[:, at])
            n_up[:, at] = new
            s_up[:, at] = state
            copies[chunk][mine] = new.astype(jnp.bfloat16)

        return run

    def step_down(h):
        def run(chunk):
            for j in range(half // LANES):
                lanes = slice(j * LANES, (j + 1) * LANES)
                at = slice(h * half + j * LANES, h * half + (j + 1) * LANES)
                new, state = update(own(chunk, lanes), turn(w_down[at, :]), turn(m_down[at, :]))
                copies[chunk][mine + (slice(None), lanes)] = new.astype(jnp.bfloat16)
                n_down[at, :] = turn(new)
                s_down[at, :] = turn(state)

        return run

    def step_query_key(chunk):
        weight = jnp.concatenate([w_query[...], w_key[...]], axis=1)
        moment = jnp.concatenate([m_query[...], m_key[...]], axis=1)
        new, state = update(own(chunk, slice(None)), weight, moment)
        copies[chunk][mine] = new.astype(jnp.bfloat16)
        n_query[...], n_key[...] = new[:, :heads], new[:, heads:]
        s_query[...], s_key[...] = state[:, :heads], state[:, heads:]

    def step_value_mixed(chunk):
        weight = jnp.concatenate([w_value[...], turn(w_mixed[...])], axis=1)
        moment = jnp.concatenate([m_value[...], turn(m_mixed[...])], axis=1)
        new, state = update(own(chunk, slice(None)), weight, moment)
        copies[chunk][mine] = new.astype(jnp.bfloat16)
        n_value[...], s_value[...] = new[:, :heads], state[:, :heads]
        n_mixed[...] = turn(new[:, heads:])
        s_mixed[...] = turn(state[:, heads:])

    def step_norm(chunk):
        new, state = update(part[chunk][mine][0:1, :rows], w_norm[...], m_norm[...])
        n_norm[...] = new
        s_norm[...] = state
        width = part[chunk].shape[-1]
        full = jnp.zeros((16, width), jnp.float32)
        if width != rows:
            new = jnp.concatenate([new, jnp.zeros((1, width - rows), jnp.float32)], axis=1)
        copies[chunk][mine] = (full + new).astype(jnp.bfloat16)

    group = 1 if rows % 16 == 0 else 2

    def end_rows(chunk, write):
        for d in range(0, n, group):
            got = [
                copies[chunk][tuple(((d + i) >> k) & 1 for k in reversed(range(bits)))] for i in range(group)
            ]
            if group > 1:
                got = [jnp.concatenate([g.astype(jnp.float32) for g in got], axis=0).astype(jnp.bfloat16)]
            write(slice(d * rows, (d + group) * rows), got[0])

    def end_up(h):
        def end(chunk):
            def write(at, value):
                c_up[at, h * half : (h + 1) * half] = value

            end_rows(chunk, write)

        return end

    def end_down(h):
        def end(chunk):
            for j in range(half // LANES):
                lanes = slice(j * LANES, (j + 1) * LANES)
                value = copies[chunk][every + (slice(None), lanes)].astype(jnp.float32)
                value = value.reshape(n * rows, LANES)
                c_down[h * half + j * LANES : h * half + (j + 1) * LANES, :] = turn(value).astype(jnp.bfloat16)

        return end

    def end_query_key(chunk):
        def write(at, value):
            value = value.astype(jnp.float32)
            c_query[at, :] = value[:, :heads].astype(jnp.bfloat16)
            c_key[at, :] = value[:, heads:].astype(jnp.bfloat16)

        end_rows(chunk, write)

    def end_value_mixed(chunk):
        def write(at, value):
            c_value[at, :] = value.astype(jnp.float32)[:, :heads].astype(jnp.bfloat16)

        end_rows(chunk, write)
        value = copies[chunk][...].astype(jnp.float32).reshape(n * rows, 2 * heads)
        c_mixed[...] = turn(value[:, heads:]).astype(jnp.bfloat16)

    def end_norm(chunk):
        got = [
            copies[chunk][tuple((d >> k) & 1 for k in reversed(range(bits)))].astype(jnp.float32)[0:1, :rows]
            for d in range(n)
        ]
        for d in range(n):
            c_norm[d : d + 1, :] = got[d]

    def fill_value_mixed(chunk):
        fill_pair(g_value, None, turn(g_mixed[...]))(chunk)

    plan = [
        (fill_up(0), step_up(0), end_up(0)),
        (fill_up(1), step_up(1), end_up(1)),
        (fill_norm, step_norm, end_norm),
        (fill_down(0), step_down(0), end_down(0)),
        (fill_down(1), step_down(1), end_down(1)),
        (fill_value_mixed, step_value_mixed, end_value_mixed),
        (fill_pair(g_query, g_key, None), step_query_key, end_query_key),
    ]

    for chunk in range(count):
        plan[chunk][0](chunk)
        scatter(chunk, 0).start()

    def event(chunk, stage):
        if stage < bits:
            scatter(chunk, stage).wait()
            where = index(chunk, stage, True)

            def body(r):
                at = pl.ds(r, SUB)
                full = where + (at, slice(None))
                lead = (slice(None),) * (len(held[chunk][stage].shape) - 2)
                part[chunk][full] = part[chunk][full] + held[chunk][stage][lead + (at, slice(None))]

            def step(i, carry):
                body(pl.multiple_of(i * SUB, SUB))
                return carry

            lax.fori_loop(0, part[chunk].shape[-2] // SUB, step, 0)
            if stage + 1 < bits:
                scatter(chunk, stage + 1).start()
            else:
                plan[chunk][1](chunk)
                gather(chunk, bits - 1).start()
        else:
            step = 2 * bits - 1 - stage
            gather(chunk, step).wait()
            if step > 0:
                gather(chunk, step - 1).start()
            else:
                plan[chunk][2](chunk)

    ahead = []
    for chunk in range(count):
        for stage in range(2 * bits):
            late = 0.5 * stage if stage < 2 * bits - 1 else max(0.5 * stage, count + 0.5 - 0.5 * chunk)
            ahead.append((chunk + late, chunk, stage))
    for _, chunk, stage in sorted(ahead):
        event(chunk, stage)


def solution(mesh):
    n = mesh.shape["data"]
    bits = n.bit_length() - 1

    def on_device(*args):
        grads, weights, moments = args[:7], args[7:14], args[14:]
        rows = weights[0].shape[0]
        grads = [g[0] for g in grads[:6]] + [grads[6].reshape(n, rows)]
        weights = list(weights[:6]) + [weights[6].reshape(1, rows)]
        moments = list(moments[:6]) + [moments[6].reshape(1, rows)]
        half, heads = grads[0].shape[1] // 2, grads[2].shape[1]
        near = tuple(range(bits))
        far = near[1:] + near[:1]
        wide = round_up(rows, LANES)
        sizes = [(rows, half)] * 2 + [(SUB, wide)] + [(rows, half)] * 2 + [(rows, 2 * heads)] * 2
        orders = [far] + [near] * 6
        copy_sizes = [s if i != 2 else (16, wide) for i, s in enumerate(sizes)]
        shape = lambda a, dtype: jax.ShapeDtypeStruct(a.shape, dtype)
        out_shape = (
            [shape(g, jnp.bfloat16) for g in grads[:6]]
            + [shape(grads[6], jnp.float32)]
            + [shape(w, jnp.float32) for w in weights]
            + [shape(w, jnp.float32) for w in weights]
        )
        scratch = [pltpu.VMEM((2,) * bits + s, jnp.float32) for s in sizes]
        for order, s in zip(orders, sizes):
            for step in range(bits):
                scratch.append(pltpu.VMEM((2,) * (bits - step - 1) + s, jnp.float32))
        scratch += [pltpu.VMEM((2,) * bits + s, jnp.bfloat16) for s in copy_sizes]
        scratch += [pltpu.SemaphoreType.DMA((len(sizes), 2 * bits))] * 2
        vmem = pl.BlockSpec(memory_space=pltpu.VMEM)
        outs = pl.pallas_call(
            functools.partial(kernel, n, bits, rows, orders),
            out_shape=out_shape,
            in_specs=[vmem] * 21,
            out_specs=[vmem] * 21,
            scratch_shapes=scratch,
            compiler_params=pltpu.CompilerParams(
                collective_id=0, has_side_effects=True, vmem_limit_bytes=60 * 2**20
            ),
        )(*grads, *weights, *moments)
        outs = list(outs)
        outs[6] = outs[6].reshape(-1).astype(jnp.bfloat16)
        outs[13] = outs[13].reshape(-1)
        outs[20] = outs[20].reshape(-1)
        return tuple(outs)

    row, col, vec = P("data", "width"), P("width", "data"), P("data")
    part = (row, col, row, row, row, col, vec)
    return jax.shard_map(
        on_device,
        mesh=mesh,
        in_specs=(
            P("data", None, "width"),
            P("data", "width", None),
            P("data", None, "width"),
            P("data", None, "width"),
            P("data", None, "width"),
            P("data", "width", None),
            P("data", None),
        )
        + part
        + part,
        out_specs=(
            P(None, "width"),
            P("width", None),
            P(None, "width"),
            P(None, "width"),
            P(None, "width"),
            P("width", None),
            P(),
        )
        + part
        + part,
        check_vma=False,
    )
```

```python
import functools

import jax
import jax.numpy as jnp
from jax import lax
from jax.experimental import pallas as pl
from jax.experimental.pallas import tpu as pltpu
from jax.sharding import PartitionSpec as P

learn_rate = 0.05
hold_rate = 0.9
LANES = 128
SUB = 8


def round_up(value, unit):
    return -(-value // unit) * unit


def turn(block):
    rows, cols = block.shape
    tall, wide = round_up(rows, LANES), round_up(cols, LANES)
    if wide != cols:
        block = jnp.concatenate([block, jnp.zeros((rows, wide - cols), block.dtype)], axis=1)
    if tall != rows:
        block = jnp.concatenate([block, jnp.zeros((tall - rows, wide), block.dtype)], axis=0)
    return block.T[:cols, :rows]


def kernel(n, bits, rows, orders, *refs):
    refs = list(refs)
    take = lambda count: [refs.pop(0) for _ in range(count)]
    g_up, g_down, g_query, g_key, g_value, g_mixed, g_norm = take(7)
    w_up, w_down, w_query, w_key, w_value, w_mixed, w_norm = take(7)
    m_up, m_down, m_query, m_key, m_value, m_mixed, m_norm = take(7)
    c_up, c_down, c_query, c_key, c_value, c_mixed, c_norm = take(7)
    n_up, n_down, n_query, n_key, n_value, n_mixed, n_norm = take(7)
    s_up, s_down, s_query, s_key, s_value, s_mixed, s_norm = take(7)
    count = len(orders)
    part = take(count)
    held = [take(bits) for _ in range(count)]
    copies = take(count)
    send_sem, recv_sem = take(2)

    me = lax.axis_index("data")
    bit = [(me // 2**k) % 2 for k in range(bits)]
    partner = [me + 2**k * (1 - 2 * bit[k]) for k in range(bits)]

    barrier = pltpu.get_barrier_semaphore()
    for k in range(bits):
        pl.semaphore_signal(
            barrier, inc=1, device_id={"data": partner[k]}, device_id_type=pl.DeviceIdType.MESH
        )
    pl.semaphore_wait(barrier, bits)

    mean_rate = n ** (-0.5)
    half = g_up.shape[1] // 2
    heads = g_query.shape[0]
    mine = tuple(bit[k] for k in reversed(range(bits)))
    every = (slice(None),) * bits

    def index(chunk, step, own):
        fixed = {k: bit[k] for k in orders[chunk][:step]}
        if step < bits:
            k = orders[chunk][step]
            fixed[k] = bit[k] if own else 1 - bit[k]
        return tuple(fixed.get(k, slice(None)) for k in reversed(range(bits)))

    def copy(src, dst, chunk, slot, k):
        return pltpu.make_async_remote_copy(
            src_ref=src,
            dst_ref=dst,
            send_sem=send_sem.at[chunk, slot],
            recv_sem=recv_sem.at[chunk, slot],
            device_id={"data": partner[k]},
            device_id_type=pl.DeviceIdType.MESH,
        )

    def scatter(chunk, step):
        return copy(
            part[chunk].at[index(chunk, step, False)],
            held[chunk][step],
            chunk,
            step,
            orders[chunk][step],
        )

    def gather(chunk, step):
        there = copies[chunk].at[index(chunk, step, True)]
        return copy(there, there, chunk, bits + step, orders[chunk][step])

    def tile_loop(body):
        def step(i, carry):
            body(pl.multiple_of(i * SUB, SUB))
            return carry

        lax.fori_loop(0, rows // SUB, step, 0)

    def blocks(value):
        return value.reshape((2,) * bits + (rows, value.shape[-1]))

    def fill_up(h):
        def fill(chunk):
            for d in range(n):
                where = tuple((d >> k) & 1 for k in reversed(range(bits)))

                def body(r):
                    part[chunk][where + (pl.ds(r, SUB), slice(None))] = g_up[
                        pl.ds(pl.multiple_of(d * rows + r, SUB), SUB), h * half : (h + 1) * half
                    ]

                tile_loop(body)

        return fill

    def fill_down(h):
        def fill(chunk):
            for j in range(half // LANES):
                block = g_down[h * half + j * LANES : h * half + (j + 1) * LANES, :]
                part[chunk][every + (slice(None), slice(j * LANES, (j + 1) * LANES))] = blocks(turn(block))

        return fill

    def fill_pair(first, second):
        def fill(chunk):
            both = turn(jnp.concatenate([first[...], second[...]], axis=0))
            part[chunk][...] = blocks(both)

        return fill

    def fill_norm(chunk):
        for d in range(n):
            where = tuple((d >> k) & 1 for k in reversed(range(bits)))
            part[chunk][where] = jnp.zeros_like(part[chunk][where])
            part[chunk][where + (slice(0, 1), slice(0, rows))] = g_norm[d : d + 1, :]

    def update(total, weight, moment):
        mean = total * mean_rate
        state = hold_rate * moment + (1.0 - hold_rate) * mean * mean
        return weight - learn_rate * mean * lax.rsqrt(state + 1e-06), state

    def own(chunk, lanes):
        return part[chunk][mine + (slice(None), lanes)]

    def step_wide(h, weight, moment, n_out, s_out):
        def run(chunk):
            at = slice(h * half, (h + 1) * half)
            new, state = update(own(chunk, slice(None)), weight[:, at], moment[:, at])
            n_out[:, at] = new
            s_out[:, at] = state
            copies[chunk][mine] = new.astype(jnp.bfloat16)

        return run

    def step_query_key(chunk):
        weight = jnp.concatenate([w_query[...], w_key[...]], axis=1)
        moment = jnp.concatenate([m_query[...], m_key[...]], axis=1)
        new, state = update(own(chunk, slice(None)), weight, moment)
        copies[chunk][mine] = new.astype(jnp.bfloat16)
        n_query[...], n_key[...] = new[:, :heads], new[:, heads:]
        s_query[...], s_key[...] = state[:, :heads], state[:, heads:]

    def step_value_mixed(chunk):
        weight = jnp.concatenate([w_value[...], turn(w_mixed[...])], axis=1)
        moment = jnp.concatenate([m_value[...], turn(m_mixed[...])], axis=1)
        new, state = update(own(chunk, slice(None)), weight, moment)
        copies[chunk][mine] = new.astype(jnp.bfloat16)
        n_value[...], s_value[...] = new[:, :heads], state[:, :heads]
        n_mixed[...] = turn(new[:, heads:])
        s_mixed[...] = turn(state[:, heads:])

    def step_norm(chunk):
        new, state = update(part[chunk][mine][0:1, :rows], w_norm[...], m_norm[...])
        n_norm[...] = new
        s_norm[...] = state
        width = part[chunk].shape[-1]
        full = jnp.zeros((16, width), jnp.float32)
        if width != rows:
            new = jnp.concatenate([new, jnp.zeros((1, width - rows), jnp.float32)], axis=1)
        copies[chunk][mine] = (full + new).astype(jnp.bfloat16)

    group = 1 if rows % 16 == 0 else 2

    def end_rows(chunk, write):
        for d in range(0, n, group):
            got = [
                copies[chunk][tuple(((d + i) >> k) & 1 for k in reversed(range(bits)))] for i in range(group)
            ]
            if group > 1:
                got = [jnp.concatenate([g.astype(jnp.float32) for g in got], axis=0).astype(jnp.bfloat16)]
            write(slice(d * rows, (d + group) * rows), got[0])

    def end_up(h):
        def end(chunk):
            def write(at, value):
                c_up[at, h * half : (h + 1) * half] = value

            end_rows(chunk, write)

        return end

    def end_down(h):
        def end(chunk):
            for j in range(half // LANES):
                lanes = slice(j * LANES, (j + 1) * LANES)
                value = copies[chunk][every + (slice(None), lanes)].astype(jnp.float32)
                value = value.reshape(n * rows, LANES)
                c_down[h * half + j * LANES : h * half + (j + 1) * LANES, :] = turn(value).astype(jnp.bfloat16)

        return end

    def end_pair(first, second):
        def end(chunk):
            value = copies[chunk][...].astype(jnp.float32).reshape(n * rows, 2 * heads)
            both = turn(value)
            first[...] = both[:heads].astype(jnp.bfloat16)
            second[...] = both[heads:].astype(jnp.bfloat16)

        return end

    def end_norm(chunk):
        got = [
            copies[chunk][tuple((d >> k) & 1 for k in reversed(range(bits)))].astype(jnp.float32)[0:1, :rows]
            for d in range(n)
        ]
        for d in range(n):
            c_norm[d : d + 1, :] = got[d]

    plan = [
        (fill_up(0), step_wide(0, w_up, m_up, n_up, s_up), end_up(0)),
        (fill_up(1), step_wide(1, w_up, m_up, n_up, s_up), end_up(1)),
        (fill_norm, step_norm, end_norm),
        (fill_down(0), step_wide(0, w_down, m_down, n_down, s_down), end_down(0)),
        (fill_down(1), step_wide(1, w_down, m_down, n_down, s_down), end_down(1)),
        (fill_pair(g_value, g_mixed), step_value_mixed, end_pair(c_value, c_mixed)),
        (fill_pair(g_query, g_key), step_query_key, end_pair(c_query, c_key)),
    ]

    for chunk in range(count):
        plan[chunk][0](chunk)
        scatter(chunk, 0).start()

    def event(chunk, stage):
        if stage < bits:
            scatter(chunk, stage).wait()
            where = index(chunk, stage, True)

            def body(r):
                at = pl.ds(r, SUB)
                full = where + (at, slice(None))
                lead = (slice(None),) * (len(held[chunk][stage].shape) - 2)
                part[chunk][full] = part[chunk][full] + held[chunk][stage][lead + (at, slice(None))]

            def step(i, carry):
                body(pl.multiple_of(i * SUB, SUB))
                return carry

            lax.fori_loop(0, part[chunk].shape[-2] // SUB, step, 0)
            if stage + 1 < bits:
                scatter(chunk, stage + 1).start()
            else:
                plan[chunk][1](chunk)
                gather(chunk, bits - 1).start()
        else:
            step = 2 * bits - 1 - stage
            gather(chunk, step).wait()
            if step > 0:
                gather(chunk, step - 1).start()
            else:
                plan[chunk][2](chunk)

    ahead = []
    for chunk in range(count):
        for stage in range(2 * bits):
            late = 0.75 * stage if stage < 2 * bits - 1 else max(0.5 * stage, count + 0.5 - 0.5 * chunk)
            ahead.append((chunk + late, chunk, stage))
    for _, chunk, stage in sorted(ahead):
        event(chunk, stage)


def hand_on(count, *refs):
    given, out, held, sem = refs[:count], refs[count : 2 * count], refs[2 * count : 3 * count], refs[3 * count]
    reads = [pltpu.make_async_copy(given[i], held[i], sem.at[0, i]) for i in range(count)]
    writes = [pltpu.make_async_copy(held[i], out[i], sem.at[1, i]) for i in range(count)]
    for read in reads:
        read.start()
    for read, write in zip(reads, writes):
        read.wait()
        write.start()
    for write in writes:
        write.wait()


def solution(mesh):
    n = mesh.shape["data"]
    bits = n.bit_length() - 1

    def on_device(*args):
        grads, weights, moments = args[:7], args[7:14], args[14:]
        rows = weights[0].shape[0]
        grads = [g[0].T if i in (2, 3, 4) else g[0] for i, g in enumerate(grads[:6])] + [grads[6].reshape(n, rows)]
        weights = list(weights[:6]) + [weights[6].reshape(1, rows)]
        moments = list(moments[:6]) + [moments[6].reshape(1, rows)]
        weights[1], moments[1] = weights[1].T, moments[1].T
        half, heads = grads[0].shape[1] // 2, grads[2].shape[0]
        near = tuple(range(bits))
        wide = round_up(rows, LANES)
        sizes = [(rows, half)] * 2 + [(SUB, wide)] + [(rows, half)] * 2 + [(rows, 2 * heads)] * 2
        orders = [near] * 7
        copy_sizes = [s if i != 2 else (16, wide) for i, s in enumerate(sizes)]
        shape = lambda a, dtype: jax.ShapeDtypeStruct(a.shape, dtype)
        out_shape = (
            [shape(g, jnp.bfloat16) for g in grads[:6]]
            + [shape(grads[6], jnp.float32)]
            + [shape(w, jnp.float32) for w in weights]
            + [shape(w, jnp.float32) for w in weights]
        )
        scratch = [pltpu.VMEM((2,) * bits + s, jnp.float32) for s in sizes]
        for order, s in zip(orders, sizes):
            for step in range(bits):
                scratch.append(pltpu.VMEM((2,) * (bits - step - 1) + s, jnp.float32))
        scratch += [pltpu.VMEM((2,) * bits + s, jnp.bfloat16) for s in copy_sizes]
        scratch += [pltpu.SemaphoreType.DMA((len(sizes), 2 * bits))] * 2
        vmem = pl.BlockSpec(memory_space=pltpu.VMEM)
        outs = pl.pallas_call(
            functools.partial(kernel, n, bits, rows, orders),
            out_shape=out_shape,
            in_specs=[vmem] * 21,
            out_specs=[vmem] * 21,
            scratch_shapes=scratch,
            compiler_params=pltpu.CompilerParams(
                collective_id=0, has_side_effects=True, vmem_limit_bytes=60 * 2**20
            ),
        )(*grads, *weights, *moments)
        count = len(outs)
        anywhere = pl.BlockSpec(memory_space=pl.ANY)
        outs = pl.pallas_call(
            functools.partial(hand_on, count),
            out_shape=out_shape,
            in_specs=[anywhere] * count,
            out_specs=[anywhere] * count,
            scratch_shapes=[pltpu.VMEM(o.shape, o.dtype) for o in out_shape] + [pltpu.SemaphoreType.DMA((2, count))],
        )(*outs)
        outs = list(outs)
        for i in (2, 3, 4, 8, 15):
            outs[i] = outs[i].T
        outs[6] = outs[6].reshape(-1).astype(jnp.bfloat16)
        outs[13] = outs[13].reshape(-1)
        outs[20] = outs[20].reshape(-1)
        return tuple(outs)

    row, col, vec = P("data", "width"), P("width", "data"), P("data")
    part = (row, col, row, row, row, col, vec)
    return jax.shard_map(
        on_device,
        mesh=mesh,
        in_specs=(
            P("data", None, "width"),
            P("data", "width", None),
            P("data", None, "width"),
            P("data", None, "width"),
            P("data", None, "width"),
            P("data", "width", None),
            P("data", None),
        )
        + part
        + part,
        out_specs=(
            P(None, "width"),
            P("width", None),
            P(None, "width"),
            P(None, "width"),
            P(None, "width"),
            P("width", None),
            P(),
        )
        + part
        + part,
        check_vma=False,
    )
```
